32 devices in a mesh: grp: 2 (over y), gx: 4 (over z), gy: 2 (over x), gz: 2 (over core).
Axes of the slice: x: 2, y: 2, z: 4, core: 2. Of those that a mesh axis runs over, the one named last changes fastest.
Arguments:
- position: float32 [64, 16, 4, 256], P(None, ('grp', 'gx'), 'gy', 'gz'), parts along dimension 1, may hold values from -6 to 6
- momentum: float32 [64, 16, 4, 256], P(None, ('grp', 'gx'), 'gy', 'gz'), parts along dimension 1, may hold values from -6 to 6
- noise: bfloat16 [3, 64, 16, 4, 256], P(None, None, ('grp', 'gx'), 'gy', 'gz'), parts along dimension 2, may hold values from -6 to 6
- filter_in: bfloat16 [64, 64, 3, 3, 3], P('gx', 'gy'), may hold values from -0.15625 to 0.15625
- filter_out: bfloat16 [64, 64, 3, 3, 3], P('gx', 'gy'), may hold values from -0.15625 to 0.15625
- bias: float32 [64], replicated, may hold values from -4 to 4
Outputs:
- final_position: float32 [64, 16, 4, 256], P(None, ('grp', 'gx'), 'gy', 'gz'), parts along dimension 1
- final_momentum: float32 [64, 16, 4, 256], P(None, ('grp', 'gx'), 'gy', 'gz'), parts along dimension 1
The draws below stay inside these ranges and needn't reach their ends.
There are 2 independent parts, one for each index of `grp`. The reference program is written for one: setup_inputs(seed, part) draws one part's arguments, and reference() takes and returns one part's arrays. A program takes and returns all parts, laid end to end along the dimension named above; an argument that names none is the same for every part. Nothing has to cross between parts.
All inputs are finite; a program needn't handle non-finite values.
Results may differ from the reference program's by a relative error of at most 0.0013.
Values may be sent and summed in bfloat16 or wider, within the bound.
A program may use at most 64 MiB of HBM per device.

```python
import jax
import jax.numpy as jnp
from jax import lax

C = 64
STEPS = 3
NX = 8
NY = 4
NZ = 256


def block_scale(own_key, shape, pieces, smallest, top_value):
    def one(axis_at, parts):
        steps = jax.random.uniform(jax.random.fold_in(jax.random.fold_in(own_key, 6), axis_at), (parts,), jnp.float32, smallest / len(pieces), top_value / len(pieces))
        return jnp.repeat(jnp.exp(steps), shape[axis_at] // parts).reshape((-1,) + (1,) * (len(shape) - axis_at - 1))

    loudness = one(*pieces[0])
    for cut in pieces[1:]:
        loudness = loudness * one(*cut)
    return loudness


def scatter_about(key, dims, scale, most, pieces=(), kind=jnp.bfloat16):
    drawn = jax.random.normal(key, dims, jnp.float32) * scale
    if len(pieces) > 0:
        drawn = block_scale(key, dims, pieces, -0.22, 0.18) * drawn
    return jnp.clip(drawn, min=-most, max=most).astype(kind)


def setup_inputs(seed: int = 0, part: int = 0) -> dict:
    streams_of = jax.random.split(jax.random.key(seed), 7)
    part_splits = jax.random.split(jax.random.fold_in(streams_of[6], part), 7)
    position = scatter_about(part_splits[0], (C, NX, NY, NZ), 1.0, 6.0, ((1, 4), (2, 2), (3, 2)), jnp.float32)
    momentum = scatter_about(part_splits[1], (C, NX, NY, NZ), 1.0, 6.0, ((1, 4), (2, 2), (3, 2)), jnp.float32)
    noise = scatter_about(part_splits[2], (STEPS, C, NX, NY, NZ), 1.0, 6.0, ((2, 4), (3, 2), (4, 2)))
    filter_in = scatter_about(streams_of[3], (C, C, 3, 3, 3), (27 * C) ** -0.5, 0.15625, ((0, 4), (1, 2)))
    filter_out = scatter_about(streams_of[4], (C, C, 3, 3, 3), (27 * C) ** -0.5, 0.15625, ((0, 4), (1, 2)))
    bias = scatter_about(streams_of[5], (C,), 1.0, 4.0, (), jnp.float32)
    return {"position": position, "momentum": momentum, "noise": noise, "filter_in": filter_in, "filter_out": filter_out, "bias": bias}


def convolve(field, filters):
    padded = jnp.pad(field, ((0, 0), (1, 1), (1, 1), (1, 1)), mode='wrap')
    return lax.conv_general_dilated(padded[None], filters, (1, 1, 1), 'VALID', dimension_numbers=('NCDHW', 'OIDHW', 'NCDHW'), preferred_element_type=jnp.float32)[0]

def adjoint(filters):
    return jnp.transpose(jnp.flip(filters, (2, 3, 4)), (1, 0, 2, 3, 4))

def reference(position, momentum, noise, filter_in, filter_out, bias):
    back_in = adjoint(filter_in)
    back_out = adjoint(filter_out)
    bias_col = bias[:, None, None, None]

    def gradient(field):
        rounded = field.astype(jnp.bfloat16)
        pre = convolve(rounded, filter_in) + bias_col
        active = jnp.tanh(pre)
        output = convolve(active.astype(jnp.bfloat16), filter_out)
        back = convolve(output.astype(jnp.bfloat16), back_out)
        hidden = (back * (1.0 - active * active)).astype(jnp.bfloat16)
        return convolve(hidden, back_in) + field
    step = 0.25
    decay = jnp.exp(jnp.float32(-0.25))
    kick = jnp.sqrt(1.0 - decay * decay)
    field = position
    moment = momentum
    force = gradient(field)
    for index in range(STEPS):
        moment = moment - 0.5 * step * force
        field = field + 0.5 * step * moment
        moment = decay * moment + kick * noise[index].astype(jnp.float32)
        field = field + 0.5 * step * moment
        force = gradient(field)
        moment = moment - 0.5 * step * force
    return (field, moment)
```

```python
import functools

import jax
import jax.numpy as jnp
from jax import lax
from jax.experimental import pallas as pl
from jax.experimental.pallas import tpu as pltpu
from jax.sharding import PartitionSpec as P

EDGE = 16
MESH = pl.DeviceIdType.MESH


def kernel(steps, sizes, pos_ref, mom_ref, noise_ref, w_ref, bias_ref,
           q_out, p_out, a1, a2, b1, b2, eq, eh, t_ref, q_ref, p_ref, send, recv, *gather):
    nx, ny, nz = sizes
    c = pos_ref.shape[0]
    inside = len(gather) > 0
    if inside:
        wg, wf, wsend, wrecv = gather
    x, z, lanes = q_ref.shape
    y = lanes // c
    full = eq.shape[1]
    wrap = ny == 2
    slots = eq.shape[2] // c
    own = slice(EDGE, EDGE + z)
    mine = slice(lanes, 2 * lanes)

    ix, iy, iz = lax.axis_index("gx"), lax.axis_index("gy"), lax.axis_index("gz")
    up = {"gx": lax.rem(ix + 1, nx), "gy": lax.rem(iy + 1, ny), "gz": lax.rem(iz + 1, nz)}
    down = {
        "gx": lax.rem(ix + nx - 1, nx),
        "gy": lax.rem(iy + ny - 1, ny),
        "gz": lax.rem(iz + nz - 1, nz),
    }

    def at_side(**which):
        return {axis: which[axis][axis] for axis in which}

    def early(buf):
        core = slice(2, 2 + x)
        low, high = slice(0, EDGE), slice(z + EDGE, full)
        block = buf.at[core, own, mine]
        edges = (
            (up, buf.at[core, z : z + EDGE, mine], low),
            (down, buf.at[core, EDGE : 2 * EDGE, mine], high),
        )
        out = []
        for side, source, rows in edges:
            out.append((at_side(gz=side), source, buf.at[core, rows, mine], True))
        for beside, part in others:
            out.append((at_side(gy=beside), block, buf.at[core, own, part], True))
            for side, source, rows in edges:
                target = buf.at[core, rows, part]
                out.append((at_side(gy=beside, gz=side), source, target, True))
        out.append((at_side(gx=up), buf.at[x : 2 + x, own, mine], buf.at[0:2, own, mine], False))
        out.append(
            (at_side(gx=down), buf.at[2:4, own, mine], buf.at[2 + x : 4 + x, own, mine], False)
        )
        return out

    def late(buf):
        low, high = slice(0, EDGE), slice(z + EDGE, full)
        areas = [(slice(0, full), part) for _, part in others] + [(low, mine), (high, mine)]
        out = []
        for rows, part in areas:
            for side, source, target in (
                (up, slice(x, 2 + x), slice(0, 2)),
                (down, slice(2, 4), slice(2 + x, 4 + x)),
            ):
                out.append(
                    (at_side(gx=side), buf.at[source, rows, part], buf.at[target, rows, part])
                )
        return out

    others = [(up, slice(0, lanes))]
    if not wrap:
        others.append((down, slice(2 * lanes, 3 * lanes)))

    def remote(source, target, sems, number, device):
        return pltpu.make_async_remote_copy(
            src_ref=source,
            dst_ref=target,
            send_sem=sems[0].at[number],
            recv_sem=sems[1].at[number],
            device_id=device,
            device_id_type=MESH,
        )

    peers = []
    if inside:
        for dx in range(nx):
            for dy in range(ny):
                if dx or dy:
                    peers.append({"gx": lax.rem(ix + dx, nx), "gy": lax.rem(iy + dy, ny)})
    barrier = pltpu.get_barrier_semaphore()
    greeted = peers + [device for device, _, _, _ in early(eq)]
    for device in greeted:
        pl.semaphore_signal(barrier, inc=1, device_id=device, device_id_type=MESH)
    pl.semaphore_wait(barrier, len(greeted))

    if inside:
        copies = []
        for number, device in enumerate(peers):
            copy = remote(w_ref, wg.at[iy, ix], (wsend, wrecv), number, device)
            copy.start()
            copies.append(copy)
        wg[iy, ix] = w_ref[...]
        for copy in copies:
            copy.wait()
        ci = c // ny
        for which in range(2):
            for at in range(27):
                columns = []
                for j in range(ny):
                    pieces = [wg[j, i, which, :, at * ci : (at + 1) * ci] for i in range(nx)]
                    columns.append(jnp.concatenate(pieces, axis=0))
                wf[which, at // 3, at % 3] = jnp.concatenate(columns, axis=1)
        filters = wf
    else:
        filters = w_ref

    def exchange(buf, bank):
        sems = (send.at[bank], recv.at[bank])
        first, own_x = [], []
        number = 0
        for device, source, target, passed in early(buf):
            copy = remote(source, target, sems, number, device)
            number += 1
            copy.start()
            (first if passed else own_x).append(copy)
        for copy in first:
            copy.wait_recv()
        second = []
        for device, source, target in late(buf):
            copy = remote(source, target, sems, number, device)
            number += 1
            copy.start()
            second.append(copy)
        for copy in own_x + second:
            copy.wait_recv()
        for copy in first + own_x + second:
            copy.wait_send()

    def slot(at):
        return at % slots

    def unfold(tap, carry):
        blank = jnp.zeros((c, c), jnp.bfloat16)

        def rows(out, which, at, flip, cols, pick):
            line = [blank] * cols
            for col, b in pick:
                line[col] = filters[which, at, 2 - b if flip else b]
            return jnp.concatenate(line, axis=1)

        back = 8 - tap
        for yo in range(y + 2):
            a1[tap, yo * c : (yo + 1) * c, :] = rows(
                a1, 0, tap, False, slots, [(slot(yo + b), b) for b in range(3)]
            )
        for yo in range(y):
            a2[tap, yo * c : (yo + 1) * c, :] = rows(
                a2, 1, tap, False, y + 2, [(yo + b, b) for b in range(3)]
            )
        for s in range(slots):
            pick = [(yo, b) for yo in range(y + 2) for b in range(3) if slot(yo + b) == s]
            b2[tap, s * c : (s + 1) * c, :] = rows(b2, 1, back, True, y + 2, pick)
        for yi in range(y + 2):
            pick = [(yo, yi - yo) for yo in range(y) if 0 <= yi - yo <= 2]
            b1[tap, yi * c : (yi + 1) * c, :] = rows(b1, 0, back, True, y, pick)
        return carry

    lax.fori_loop(0, 9, unfold, 0)

    def load(ref2d, at):
        span = [ref2d[:, (at * y + j) * z : (at * y + j + 1) * z] for j in range(y)]
        return jnp.concatenate(span, axis=0).astype(jnp.float32).T

    for at in range(x):
        q_ref[at] = load(pos_ref, at)
        p_ref[at] = load(mom_ref, at)

    def conv(source, weights, out_x, transposed):
        width = source.shape[2]
        total = None
        for tz in range(3):
            part = None
            for tx in range(3):
                left = source[tx : tx + out_x].reshape(out_x * full, width)
                term = lax.dot_general(
                    left,
                    weights[tx * 3 + tz],
                    (((1,), (1 if transposed else 0,)), ((), ())),
                    preferred_element_type=jnp.float32,
                )
                part = term if part is None else part + term
            if tz != 1:
                part = pltpu.roll(part, 1 if tz == 0 else out_x * full - 1, 0)
            total = part if total is None else total + part
        return total.reshape(out_x, full, total.shape[-1])

    step = 0.25
    decay = jnp.exp(jnp.float32(-0.25))
    kick = jnp.sqrt(1.0 - decay * decay)

    def body(k, carry):
        eq[2 : 2 + x, own, mine] = q_ref[...].astype(jnp.bfloat16)
        exchange(eq, 0)
        t_ref[...] = jnp.tanh(conv(eq, a1, x + 2, True) + bias_ref[...][None])
        h2 = conv(t_ref[...].astype(jnp.bfloat16), a2, x, True)
        eh[2 : 2 + x, own, mine] = h2[:, own].astype(jnp.bfloat16)
        exchange(eh, 1)
        gu = conv(eh, b2, x + 2, False)
        t = t_ref[...]
        gh = (gu * (1.0 - t * t)).astype(jnp.bfloat16)
        force = conv(gh, b1, x, False)[:, own] + q_ref[...]
        half = 0.5 * step

        @pl.when(k > 0)
        def _():
            p_ref[...] = p_ref[...] - half * force

        @pl.when(k < steps)
        def _():
            p = p_ref[...] - half * force
            q = q_ref[...] + half * p
            now = noise_ref.at[k]
            drawn = jnp.stack([load(now, at) for at in range(x)])
            p = decay * p + kick * drawn
            q_ref[...] = q + half * p
            p_ref[...] = p

        return carry

    lax.fori_loop(0, steps + 1, body, 0)

    for ref, out in ((q_ref, q_out), (p_ref, p_out)):
        for at in range(x):
            flat = ref[at].T
            for j in range(y):
                out[:, (at * y + j) * z : (at * y + j + 1) * z] = flat[j * c : (j + 1) * c]


def on_device(sizes, position, momentum, noise, filter_in, filter_out, bias):
    nx, ny, nz = sizes
    c, x, y, z = position.shape
    steps = noise.shape[0]
    assert x >= 2 and y == 2 and z % EDGE == 0 and nx > 2 and ny > 1
    both = jnp.stack([filter_in, filter_out])
    co, ci = both.shape[1], both.shape[2]
    gather = []
    if co % EDGE == 0:
        both = both.transpose(0, 1, 3, 5, 4, 2).reshape(2, co, 27 * ci)
        gather = [
            pltpu.VMEM((ny, nx, 2, co, 27 * ci), jnp.bfloat16),
            pltpu.VMEM((2, 9, 3, c, c), jnp.bfloat16),
            pltpu.SemaphoreType.DMA((nx * ny - 1,)),
            pltpu.SemaphoreType.DMA((nx * ny - 1,)),
        ]
    else:
        both = both.reshape(2 * co, ci * 27)
        both = lax.all_gather(both, ("gx", "gy"), axis=0, tiled=True)
        both = both.reshape(nx, ny, 2, co, ci, 3, 3, 3)
        both = both.transpose(2, 5, 7, 6, 0, 3, 1, 4).reshape(2, 9, 3, c, c)
    lanes = y * c
    slots = 2 * y if ny == 2 else 3 * y
    full = z + 2 * EDGE
    wide = (y + 2) * c
    flat = jax.ShapeDtypeStruct((c, x * y * z), jnp.float32)
    copies = 13 if ny == 2 else 18
    vmem = pl.BlockSpec(memory_space=pltpu.VMEM)
    q, p = pl.pallas_call(
        functools.partial(kernel, steps, sizes),
        out_shape=(flat, flat),
        in_specs=[vmem] * 5,
        out_specs=(vmem, vmem),
        scratch_shapes=[
            pltpu.VMEM((9, wide, slots * c), jnp.bfloat16),
            pltpu.VMEM((9, lanes, wide), jnp.bfloat16),
            pltpu.VMEM((9, wide, lanes), jnp.bfloat16),
            pltpu.VMEM((9, slots * c, wide), jnp.bfloat16),
            pltpu.VMEM((x + 4, full, slots * c), jnp.bfloat16),
            pltpu.VMEM((x + 4, full, slots * c), jnp.bfloat16),
            pltpu.VMEM((x + 2, full, wide), jnp.float32),
            pltpu.VMEM((x, z, lanes), jnp.float32),
            pltpu.VMEM((x, z, lanes), jnp.float32),
            pltpu.SemaphoreType.DMA((2, copies)),
            pltpu.SemaphoreType.DMA((2, copies)),
            *gather,
        ],
        compiler_params=pltpu.CompilerParams(
            collective_id=0, has_side_effects=True, vmem_limit_bytes=56 * 2**20
        ),
    )(
        position.reshape(c, -1),
        momentum.reshape(c, -1),
        noise.reshape(steps, c, -1),
        both,
        jnp.tile(bias, y + 2)[None],
    )
    return q.reshape(position.shape), p.reshape(momentum.shape)


def solution(mesh):
    field = P(None, ("grp", "gx"), "gy", "gz")
    filters = P("gx", "gy", None, None, None)
    sizes = tuple(mesh.shape[name] for name in ("gx", "gy", "gz"))
    return jax.shard_map(
        functools.partial(on_device, sizes),
        mesh=mesh,
        in_specs=(field, field, P(None, None, ("grp", "gx"), "gy", "gz"), filters, filters, P()),
        out_specs=(field, field),
        check_vma=False,
    )
```

```python
import functools

import jax
import jax.numpy as jnp
from jax import lax
from jax.experimental import pallas as pl
from jax.experimental.pallas import tpu as pltpu
from jax.sharding import PartitionSpec as P

EDGE = 16
MESH = pl.DeviceIdType.MESH


def kernel(steps, sizes, pos_ref, mom_ref, noise_ref, w_ref, bias_ref,
           q_out, p_out, a1, a2, b1, b2, eq, eh, t_ref, q_ref, p_ref, send, recv, *gather):
    nx, ny, nz = sizes
    c = pos_ref.shape[0]
    inside = len(gather) > 0
    if inside:
        wg, wf, wsend, wrecv = gather
    x, z, lanes = q_ref.shape
    y = lanes // c
    full = eq.shape[1]
    wrap = ny == 2
    slots = eq.shape[2] // c
    own = slice(EDGE, EDGE + z)
    mine = slice(lanes, 2 * lanes)

    ix, iy, iz = lax.axis_index("gx"), lax.axis_index("gy"), lax.axis_index("gz")
    up = {"gx": lax.rem(ix + 1, nx), "gy": lax.rem(iy + 1, ny), "gz": lax.rem(iz + 1, nz)}
    down = {
        "gx": lax.rem(ix + nx - 1, nx),
        "gy": lax.rem(iy + ny - 1, ny),
        "gz": lax.rem(iz + nz - 1, nz),
    }

    def at_side(**which):
        return {axis: which[axis][axis] for axis in which}

    def early(buf):
        core = slice(2, 2 + x)
        low, high = slice(0, EDGE), slice(z + EDGE, full)
        block = buf.at[core, own, mine]
        edges = (
            (up, buf.at[core, z : z + EDGE, mine], low),
            (down, buf.at[core, EDGE : 2 * EDGE, mine], high),
        )
        out = []
        for side, source, rows in edges:
            out.append((at_side(gz=side), source, buf.at[core, rows, mine], True))
        for beside, part in others:
            out.append((at_side(gy=beside), block, buf.at[core, own, part], True))
            for side, source, rows in edges:
                target = buf.at[core, rows, part]
                out.append((at_side(gy=beside, gz=side), source, target, True))
        out.append(
            (at_side(gx=down), buf.at[2:4, own, mine], buf.at[2 + x : 4 + x, own, mine], False)
        )
        out.append((at_side(gx=up), buf.at[x : 2 + x, own, mine], buf.at[0:2, own, mine], False))
        return out

    def late(buf):
        low, high = slice(0, EDGE), slice(z + EDGE, full)
        from_low = (up, slice(x, 2 + x), slice(0, 2))
        from_high = (down, slice(2, 4), slice(2 + x, 4 + x))
        plan = []
        for _, part in others:
            plan.append((from_low, slice(0, full), part))
            plan += [(from_high, low, part), (from_high, high, part)]
        for side in (from_low, from_high):
            plan += [(side, low, mine), (side, high, mine)]
        return [
            (at_side(gx=side), buf.at[source, rows, part], buf.at[target, rows, part])
            for (side, source, target), rows, part in plan
        ]

    def forward(buf):
        planes = slice(2 + x, 4 + x)
        return [
            (at_side(gy=beside), buf.at[planes, own, mine], buf.at[planes, own, part])
            for beside, part in others
        ]

    others = [(up, slice(0, lanes))]
    if not wrap:
        others.append((down, slice(2 * lanes, 3 * lanes)))

    def remote(source, target, sems, number, device):
        return pltpu.make_async_remote_copy(
            src_ref=source,
            dst_ref=target,
            send_sem=sems[0].at[number],
            recv_sem=sems[1].at[number],
            device_id=device,
            device_id_type=MESH,
        )

    peers = []
    if inside:
        for dx in range(nx):
            for dy in range(ny):
                if dx or dy:
                    peers.append({"gx": lax.rem(ix + dx, nx), "gy": lax.rem(iy + dy, ny)})
    barrier = pltpu.get_barrier_semaphore()
    greeted = peers + [device for device, _, _, _ in early(eq)]
    for device in greeted:
        pl.semaphore_signal(barrier, inc=1, device_id=device, device_id_type=MESH)
    pl.semaphore_wait(barrier, len(greeted))

    if inside:
        copies = []
        for number, device in enumerate(peers):
            copy = remote(w_ref, wg.at[iy, ix], (wsend, wrecv), number, device)
            copy.start()
            copies.append(copy)
        wg[iy, ix] = w_ref[...]
        for copy in copies:
            copy.wait()
        ci = c // ny
        for which in range(2):
            for at in range(27):
                columns = []
                for j in range(ny):
                    pieces = [wg[j, i, which, :, at * ci : (at + 1) * ci] for i in range(nx)]
                    columns.append(jnp.concatenate(pieces, axis=0))
                wf[which, at // 3, at % 3] = jnp.concatenate(columns, axis=1)
        filters = wf
    else:
        filters = w_ref

    def exchange(buf, bank):
        sems = (send.at[bank], recv.at[bank])
        first, own_x = [], []
        number = 0
        for device, source, target, passed in early(buf):
            copy = remote(source, target, sems, number, device)
            number += 1
            copy.start()
            (first if passed else own_x).append(copy)
        for copy in first:
            copy.wait_recv()
        second = []
        for device, source, target in late(buf):
            copy = remote(source, target, sems, number, device)
            number += 1
            copy.start()
            second.append(copy)
        own_x[0].wait_recv()
        for device, source, target in forward(buf):
            copy = remote(source, target, sems, number, device)
            number += 1
            copy.start()
            second.append(copy)
        for copy in own_x[1:] + second:
            copy.wait_recv()
        for copy in first + own_x + second:
            copy.wait_send()

    def slot(at):
        return at % slots

    def unfold(tap, carry):
        blank = jnp.zeros((c, c), jnp.bfloat16)

        def rows(out, which, at, flip, cols, pick):
            line = [blank] * cols
            for col, b in pick:
                line[col] = filters[which, at, 2 - b if flip else b]
            return jnp.concatenate(line, axis=1)

        back = 8 - tap
        for yo in range(y + 2):
            a1[tap, yo * c : (yo + 1) * c, :] = rows(
                a1, 0, tap, False, slots, [(slot(yo + b), b) for b in range(3)]
            )
        for yo in range(y):
            a2[tap, yo * c : (yo + 1) * c, :] = rows(
                a2, 1, tap, False, y + 2, [(yo + b, b) for b in range(3)]
            )
        for s in range(slots):
            pick = [(yo, b) for yo in range(y + 2) for b in range(3) if slot(yo + b) == s]
            b2[tap, s * c : (s + 1) * c, :] = rows(b2, 1, back, True, y + 2, pick)
        for yi in range(y + 2):
            pick = [(yo, yi - yo) for yo in range(y) if 0 <= yi - yo <= 2]
            b1[tap, yi * c : (yi + 1) * c, :] = rows(b1, 0, back, True, y, pick)
        return carry

    lax.fori_loop(0, 9, unfold, 0)

    def load(ref2d, at):
        span = [ref2d[:, (at * y + j) * z : (at * y + j + 1) * z] for j in range(y)]
        return jnp.concatenate(span, axis=0).astype(jnp.float32).T

    for at in range(x):
        q_ref[at] = load(pos_ref, at)
        p_ref[at] = load(mom_ref, at)

    def conv(source, weights, out_x, transposed):
        width = source.shape[2]
        total = None
        for tz in range(3):
            part = None
            for tx in range(3):
                left = source[tx : tx + out_x].reshape(out_x * full, width)
                term = lax.dot_general(
                    left,
                    weights[tx * 3 + tz],
                    (((1,), (1 if transposed else 0,)), ((), ())),
                    preferred_element_type=jnp.float32,
                )
                part = term if part is None else part + term
            if tz != 1:
                part = pltpu.roll(part, 1 if tz == 0 else out_x * full - 1, 0)
            total = part if total is None else total + part
        return total.reshape(out_x, full, total.shape[-1])

    step = 0.25
    decay = jnp.exp(jnp.float32(-0.25))
    kick = jnp.sqrt(1.0 - decay * decay)

    def body(k, carry):
        eq[2 : 2 + x, own, mine] = q_ref[...].astype(jnp.bfloat16)
        exchange(eq, 0)
        t_ref[...] = jnp.tanh(conv(eq, a1, x + 2, True) + bias_ref[...][None])
        h2 = conv(t_ref[...].astype(jnp.bfloat16), a2, x, True)
        eh[2 : 2 + x, own, mine] = h2[:, own].astype(jnp.bfloat16)
        exchange(eh, 1)
        gu = conv(eh, b2, x + 2, False)
        t = t_ref[...]
        gh = (gu * (1.0 - t * t)).astype(jnp.bfloat16)
        force = conv(gh, b1, x, False)[:, own] + q_ref[...]
        half = 0.5 * step

        @pl.when(k > 0)
        def _():
            p_ref[...] = p_ref[...] - half * force

        @pl.when(k < steps)
        def _():
            p = p_ref[...] - half * force
            q = q_ref[...] + half * p
            now = noise_ref.at[k]
            drawn = jnp.stack([load(now, at) for at in range(x)])
            p = decay * p + kick * drawn
            q_ref[...] = q + half * p
            p_ref[...] = p

        return carry

    lax.fori_loop(0, steps + 1, body, 0)

    for ref, out in ((q_ref, q_out), (p_ref, p_out)):
        for at in range(x):
            flat = ref[at].T
            for j in range(y):
                out[:, (at * y + j) * z : (at * y + j + 1) * z] = flat[j * c : (j + 1) * c]


def on_device(sizes, position, momentum, noise, filter_in, filter_out, bias):
    nx, ny, nz = sizes
    c, x, y, z = position.shape
    steps = noise.shape[0]
    assert x >= 2 and y == 2 and z % EDGE == 0 and nx > 2 and ny > 1
    both = jnp.stack([filter_in, filter_out])
    co, ci = both.shape[1], both.shape[2]
    gather = []
    if co % EDGE == 0:
        both = both.transpose(0, 1, 3, 5, 4, 2).reshape(2, co, 27 * ci)
        gather = [
            pltpu.VMEM((ny, nx, 2, co, 27 * ci), jnp.bfloat16),
            pltpu.VMEM((2, 9, 3, c, c), jnp.bfloat16),
            pltpu.SemaphoreType.DMA((nx * ny - 1,)),
            pltpu.SemaphoreType.DMA((nx * ny - 1,)),
        ]
    else:
        both = both.reshape(2 * co, ci * 27)
        both = lax.all_gather(both, ("gx", "gy"), axis=0, tiled=True)
        both = both.reshape(nx, ny, 2, co, ci, 3, 3, 3)
        both = both.transpose(2, 5, 7, 6, 0, 3, 1, 4).reshape(2, 9, 3, c, c)
    lanes = y * c
    slots = 2 * y if ny == 2 else 3 * y
    full = z + 2 * EDGE
    wide = (y + 2) * c
    flat = jax.ShapeDtypeStruct((c, x * y * z), jnp.float32)
    copies = 15 if ny == 2 else 24
    vmem = pl.BlockSpec(memory_space=pltpu.VMEM)
    q, p = pl.pallas_call(
        functools.partial(kernel, steps, sizes),
        out_shape=(flat, flat),
        in_specs=[vmem] * 5,
        out_specs=(vmem, vmem),
        scratch_shapes=[
            pltpu.VMEM((9, wide, slots * c), jnp.bfloat16),
            pltpu.VMEM((9, lanes, wide), jnp.bfloat16),
            pltpu.VMEM((9, wide, lanes), jnp.bfloat16),
            pltpu.VMEM((9, slots * c, wide), jnp.bfloat16),
            pltpu.VMEM((x + 4, full, slots * c), jnp.bfloat16),
            pltpu.VMEM((x + 4, full, slots * c), jnp.bfloat16),
            pltpu.VMEM((x + 2, full, wide), jnp.float32),
            pltpu.VMEM((x, z, lanes), jnp.float32),
            pltpu.VMEM((x, z, lanes), jnp.float32),
            pltpu.SemaphoreType.DMA((2, copies)),
            pltpu.SemaphoreType.DMA((2, copies)),
            *gather,
        ],
        compiler_params=pltpu.CompilerParams(
            collective_id=0, has_side_effects=True, vmem_limit_bytes=56 * 2**20
        ),
    )(
        position.reshape(c, -1),
        momentum.reshape(c, -1),
        noise.reshape(steps, c, -1),
        both,
        jnp.tile(bias, y + 2)[None],
    )
    return q.reshape(position.shape), p.reshape(momentum.shape)


def solution(mesh):
    field = P(None, ("grp", "gx"), "gy", "gz")
    filters = P("gx", "gy", None, None, None)
    sizes = tuple(mesh.shape[name] for name in ("gx", "gy", "gz"))
    return jax.shard_map(
        functools.partial(on_device, sizes),
        mesh=mesh,
        in_specs=(field, field, P(None, None, ("grp", "gx"), "gy", "gz"), filters, filters, P()),
        out_specs=(field, field),
        check_vma=False,
    )
```
